128 devices in a mesh: dp: 8 (over z_hi, y), mp: 16 (over x, z_lo, core).
Axes of the slice: x: 4, y: 4, z: 4 (z_hi: 2, z_lo: 2; z = z_hi * 2 + z_lo), core: 2. Of those that a mesh axis runs over, the one named last changes fastest.
Arguments:
- teacher_in: bfloat16 [8192, 6144], P('dp'), may hold values from -60 to 60
- w_query: bfloat16 [6144, 6144], P('dp', 'mp'), may hold values from -0.109375 to 0.109375
- w_key: bfloat16 [6144, 6144], P('dp', 'mp'), may hold values from -0.109375 to 0.109375
- w_value: bfloat16 [6144, 6144], P('dp', 'mp'), may hold values from -0.625 to 0.625
- student_in: bfloat16 [8192, 1024], P(('dp', 'mp')), may hold values from -24 to 24
- norm_gain: float32 [1024], replicated, may hold values from 0.5 to 1.5
- norm_bias: float32 [1024], replicated, may hold values from -3 to 3
- head_weight: bfloat16 [1024, 6144], P(None, 'mp'), may hold values from -0.1875 to 0.1875
- head_bias: bfloat16 [6144], P('mp'), may hold values from -3 to 3
Outputs:
- grad_head_w: float32 [1024, 6144], P('dp', 'mp')
- grad_head_b: float32 [6144], P('mp')
- grad_gain: float32 [1024], replicated
- grad_bias: float32 [1024], replicated
- grad_in: float32 [8192, 1024], P(('dp', 'mp'))
The draws below stay inside these ranges and needn't reach their ends.
All inputs are finite; a program needn't handle non-finite values.
Results may differ from the reference program's by a relative error of at most 0.0094.
Values may be sent and summed in bfloat16 or wider, within the bound.
No kernel may reach another device: no remote copies, remote signals or barrier semaphores. Data moves between devices by JAX's collectives and lax.ppermute only.
A program may use at most 128 MiB of HBM per device.

```python
import jax
import jax.numpy as jnp
from jax import lax

D_T = 6144
HEADS = 48
HEAD_DIM = 128
D_S = 1024
IMAGE_TOK = 256
TOKENS = 8192


def draw_teacher_in(key, part):
    first = jax.random.fold_in(jax.random.fold_in(key, 11), 0)
    base = jnp.clip(jax.random.normal(first, (TOKENS, D_T), jnp.float32), -6.0, 6.0)
    return base.astype(jnp.bfloat16)


def with_spikes(array, key, source, target, blocks, factor):
    owner, partner = [(jnp.arange(array.shape[position]) // (array.shape[position] // blocks)).reshape([-1 if axis == position else 1 for axis in range(array.ndim)]) for position in (source, target)]
    chosen = jax.random.permutation(key, blocks)[partner]
    strong = (owner == chosen) | (owner == (partner + blocks // 2) % blocks)
    return jnp.where(strong, factor * array, array)


def level_of(own_key, dims, shards, low, largest):
    level = 1.0
    for axis_at, shards_of in shards:
        draws = jax.random.uniform(jax.random.fold_in(jax.random.fold_in(own_key, 6), axis_at), (shards_of,), jnp.float32, low / len(shards), largest / len(shards))
        level = level * jnp.repeat(jnp.exp(draws), dims[axis_at] // shards_of).reshape((-1,) + (1,) * (len(dims) - 1 - axis_at))
    return level


def noise(stream_key, shape, deviation, bound, pieces=(), kind=jnp.bfloat16):
    values = jax.random.normal(stream_key, shape, jnp.float32) * deviation
    if len(pieces) > 0:
        values = level_of(stream_key, shape, pieces, -0.22, 0.18) * values
    return jnp.clip(values, min=-bound, max=bound).astype(kind)


def noise_with(own_key, dims, deviation, most, pieces, heavy, kind=jnp.bfloat16):
    values = deviation * jax.random.normal(own_key, dims, jnp.float32)
    if pieces:
        values = values * level_of(own_key, dims, pieces, -0.22, 0.18)
    return jnp.clip(with_spikes(values, jax.random.fold_in(own_key, 3), *heavy), -most, most).astype(kind)


def setup_inputs(seed: int = 0) -> dict:
    seeds = jax.random.split(jax.random.key(seed), 10)
    return {
        "teacher_in": draw_teacher_in(jax.random.fold_in(seeds[9], 71), 0),
        "w_query": noise(seeds[1], (D_T, D_T), (D_T // 2) ** -0.5, 0.109375, ((0, 8), (1, 16))),
        "w_key": noise(seeds[2], (D_T, D_T), (D_T // 2) ** -0.5, 0.109375, ((0, 8), (1, 16))),
        "w_value": noise(seeds[3], (D_T, D_T), (D_T // 64) ** -0.5, 0.625, ((0, 8), (1, 16))),
        "student_in": noise_with(seeds[4], (TOKENS, D_S), 1.0, 24.0, ((0, 128),), (0, 1, 128, 5.5)),
        "norm_gain": jnp.clip(1.0 + 0.1 * jax.random.normal(seeds[5], (D_S,), jnp.float32), 0.5, 1.5),
        "norm_bias": noise(seeds[6], (D_S,), 0.5, 3.0, (), jnp.float32),
        "head_weight": noise(seeds[7], (D_S, D_T), D_S ** -0.5, 0.1875, ((1, 16),)),
        "head_bias": noise(seeds[8], (D_T,), 0.5, 3.0, ((0, 16),)),
    }


def reference(teacher_in, w_query, w_key, w_value, student_in, norm_gain, norm_bias, head_weight, head_bias):
    query = jnp.dot(teacher_in, w_query, preferred_element_type=jnp.float32).astype(jnp.bfloat16)
    keys = jnp.dot(teacher_in, w_key, preferred_element_type=jnp.float32).astype(jnp.bfloat16)
    values = jnp.dot(teacher_in, w_value, preferred_element_type=jnp.float32).astype(jnp.bfloat16)
    images = query.shape[0] // IMAGE_TOK

    def split(block):
        return block.reshape(images, IMAGE_TOK, HEADS, HEAD_DIM).astype(jnp.float32)
    scores = jnp.einsum('bqhd,bkhd->bhqk', split(query), split(keys)) * HEAD_DIM ** (-0.5)
    top = lax.optimization_barrier(jnp.max(scores, axis=-1, keepdims=True))
    weights = jnp.exp(scores - top)
    probs = (weights / lax.optimization_barrier(jnp.sum(weights, axis=-1, keepdims=True))).astype(jnp.bfloat16)
    feats = jnp.einsum('bhqk,bkhd->bqhd', probs.astype(jnp.float32), split(values))
    feats = feats.reshape(query.shape[0], HEADS * HEAD_DIM).astype(jnp.bfloat16)
    student = student_in.astype(jnp.float32)
    center = student - lax.optimization_barrier(jnp.mean(student, axis=-1, keepdims=True))
    inverse = lax.rsqrt(lax.optimization_barrier(jnp.mean(center * center, axis=-1, keepdims=True)) + 1e-06)
    core = center * inverse
    normed = (core * norm_gain + norm_bias).astype(jnp.bfloat16)
    output = jnp.dot(normed, head_weight, preferred_element_type=jnp.float32) + head_bias.astype(jnp.float32)
    scale = float(TOKENS) ** (-0.5)
    error = ((output - feats.astype(jnp.float32)) * scale).astype(jnp.bfloat16)
    grad_head_w = jnp.dot(normed.T, error, preferred_element_type=jnp.float32)
    grad_head_b = lax.optimization_barrier(jnp.sum(error.astype(jnp.float32), axis=0))
    grad_normed = jnp.dot(error, head_weight.T, preferred_element_type=jnp.float32)
    grad_gain = lax.optimization_barrier(jnp.sum(grad_normed * core, axis=0))
    grad_bias = lax.optimization_barrier(jnp.sum(grad_normed, axis=0))
    grad_core = grad_normed * norm_gain
    grad_in = inverse * (grad_core - lax.optimization_barrier(jnp.mean(grad_core, axis=-1, keepdims=True)) - core * lax.optimization_barrier(jnp.mean(grad_core * core, axis=-1, keepdims=True)))
    return (grad_head_w, grad_head_b, grad_gain, grad_bias, grad_in)
```

```python
import functools

import jax
import jax.numpy as jnp
from jax import lax
from jax.experimental import pallas as pl
from jax.experimental.pallas import tpu as pltpu
from jax.sharding import Mesh, PartitionSpec as P

HEAD_DIM = 128
IMAGE_TOK = 256
BF16 = jnp.bfloat16
F32 = jnp.float32


def moved(array, axis, step):
    n = lax.axis_size(axis)
    return lax.ppermute(array, axis, [(i, (i + step) % n) for i in range(n)])


def tied(value, *after):
    return lax.optimization_barrier((value, *after))[0]


def probs_kernel(q_ref, k_ref, p_ref):
    scores = lax.dot_general(
        q_ref[...], k_ref[...], (((1,), (1,)), ((), ())), preferred_element_type=F32
    ) * (HEAD_DIM ** (-0.5))
    top = jnp.max(scores, axis=-1, keepdims=True)
    weights = jnp.exp(scores - top)
    p_ref[0, 0] = (weights / jnp.sum(weights, axis=-1, keepdims=True)).astype(BF16)


def probs_of(query, keys):
    tokens, width = query.shape
    images, heads = tokens // IMAGE_TOK, width // HEAD_DIM
    spec = pl.BlockSpec((IMAGE_TOK, HEAD_DIM), lambda i, h: (i, h))
    return pl.pallas_call(
        probs_kernel,
        grid=(images, heads),
        in_specs=[spec, spec],
        out_specs=pl.BlockSpec((1, 1, IMAGE_TOK, IMAGE_TOK), lambda i, h: (i, h, 0, 0)),
        out_shape=jax.ShapeDtypeStruct((images, heads, IMAGE_TOK, IMAGE_TOK), BF16),
        cost_estimate=pl.CostEstimate(
            flops=2 * tokens * IMAGE_TOK * width * 8, bytes_accessed=0, transcendentals=0
        ),
    )(query, keys)


def error_kernel(scale, p_ref, v_ref, o_ref, e_ref):
    feats = jnp.dot(p_ref[0, 0], v_ref[...].astype(BF16), preferred_element_type=F32)
    e_ref[...] = ((o_ref[...] - feats.astype(BF16).astype(F32)) * scale).astype(BF16)


def error_of(probs, values, output, scale):
    tokens, width = values.shape
    images, heads = probs.shape[:2]
    spec = pl.BlockSpec((IMAGE_TOK, HEAD_DIM), lambda i, h: (i, h))
    return pl.pallas_call(
        functools.partial(error_kernel, scale),
        grid=(images, heads),
        in_specs=[
            pl.BlockSpec((1, 1, IMAGE_TOK, IMAGE_TOK), lambda i, h: (i, h, 0, 0)),
            spec,
            spec,
        ],
        out_specs=spec,
        out_shape=jax.ShapeDtypeStruct((tokens, width), BF16),
        cost_estimate=pl.CostEstimate(
            flops=2 * tokens * IMAGE_TOK * width, bytes_accessed=0, transcendentals=0
        ),
    )(probs, values, output)


def on_device(
    teacher_in, w_query, w_key, w_value, student_in, norm_gain, norm_bias, head_weight, head_bias
):
    zh, y, x, zl, c = (lax.axis_index(a) for a in ("zh", "y", "x", "zl", "c"))
    tokens = teacher_in.shape[0]
    depth, width = w_query.shape
    d_s = head_weight.shape[0]
    scale = float(tokens * 8) ** (-0.5)

    def rows_of(z_at, y_at):
        start = (z_at * 4 + y_at % 4) * depth
        return lax.dynamic_slice_in_dim(teacher_in, start, depth, axis=1)

    weights = (w_query, w_key, w_value)
    ahead, behind, across = [], [], []
    for w in weights:
        behind.append(moved(w, "y", 1))
        ahead.append(moved(w, "y", -1))
        across.append(moved(w, "zh", 1))

    student = student_in.astype(F32)
    center = student - jnp.mean(student, axis=-1, keepdims=True)
    inverse = lax.rsqrt(jnp.mean(center * center, axis=-1, keepdims=True) + 1e-06)
    core = center * inverse
    own = core.astype(BF16)
    rows = own.shape[0]
    other_zl = moved(own, "zl", 1)
    pair = jnp.where(zl == 0, jnp.stack([own, other_zl]), jnp.stack([other_zl, own]))
    buf = jnp.zeros((4, 2, 2, rows, d_s), BF16)
    for dx in range(4):
        got = pair if dx == 0 else moved(pair, "x", dx)
        buf = lax.dynamic_update_slice(buf, got[None, :, None], ((x - dx) % 4, 0, c, 0, 0))
    mine = lax.dynamic_slice(buf, (0, 0, c, 0, 0), (4, 2, 1, rows, d_s))
    theirs = moved(mine, "c", 1)
    buf = lax.dynamic_update_slice(buf, theirs, (0, 0, 1 - c, 0, 0))
    cores = buf.reshape(tokens, d_s)
    normed = (cores.astype(F32) * norm_gain + norm_bias).astype(BF16)
    output = jnp.dot(normed, head_weight, preferred_element_type=F32) + head_bias.astype(F32)

    heads_same = [head_weight] + [moved(head_weight, "x", dx) for dx in range(1, 4)]
    heads_swap = [moved(h, "c", 1) for h in heads_same]

    def pick(even, odd):
        return jnp.where(c == 0, even, odd)

    def ring(pairs):
        perm = []
        for i in range(4):
            perm.append((i * 2, ((i + 1) % 4) * 2))
            perm.append((i * 2 + 1, ((i - 1) % 4) * 2 + 1))
        return lax.ppermute(pairs, ("y", "c"), perm)

    opposite = [ring(pick(b, a)) for b, a in zip(behind, ahead)]
    far_opposite = [moved(o, "zh", 1) for o in opposite]
    far_behind, far_ahead = [], []
    for i in range(2):
        far_behind.append(moved(across[i], "y", 1))
        far_ahead.append(moved(across[i], "y", -1))
    by_y = ring(across[2])
    by_z = moved(pick(ahead[2], behind[2]), "zh", 1)

    side = jnp.where(c == 0, 1, -1)
    a_own = rows_of(zh, y)
    a_ahead = rows_of(zh, y + 1)
    a_behind = rows_of(zh, y + 3)
    a_opp = rows_of(zh, y + 2)
    f_own = rows_of(1 - zh, y)
    f_ahead = rows_of(1 - zh, y + 1)
    f_behind = rows_of(1 - zh, y + 3)
    f_opp = rows_of(1 - zh, y + 2)
    f_by_y = rows_of(1 - zh, y + 4 - side)
    f_by_z = rows_of(1 - zh, y + 4 + side)

    def total(terms):
        out = None
        for a, w in terms:
            term = jnp.dot(a, w, preferred_element_type=F32)
            out = term if out is None else out + term
        return out

    def first_terms(i):
        return [
            (a_own, weights[i]),
            (a_behind, behind[i]),
            (a_ahead, ahead[i]),
            (f_own, across[i]),
            (a_opp, opposite[i]),
        ]

    query, keys = (
        total(
            first_terms(i)
            + [
                (f_opp, far_opposite[i]),
                (f_behind, far_behind[i]),
                (f_ahead, far_ahead[i]),
            ]
        ).astype(BF16)
        for i in range(2)
    )
    values = total(first_terms(2) + [(f_by_z, by_z), (f_opp, far_opposite[2]), (f_by_y, by_y)])

    probs = probs_of(query, keys)
    error = error_of(probs, values, output, scale)

    blocks = error.reshape(4, 2, 2, rows, width)
    grad_part = None
    for dx in range(4):
        for dc in range(2):
            block = lax.dynamic_slice(
                blocks, ((x + dx) % 4, 0, (c + dc) % 2, 0, 0), (1, 2, 1, rows, width)
            ).reshape(2 * rows, width)
            if dx or dc:
                perm = [
                    (i * 2 + j, ((i + dx) % 4) * 2 + (j + dc) % 2)
                    for i in range(4)
                    for j in range(2)
                ]
                block = lax.ppermute(block, ("x", "c"), perm)
            head = heads_swap[dx] if dc else heads_same[dx]
            term = lax.dot_general(
                block, head, (((1,), (1,)), ((), ())), preferred_element_type=F32
            )
            grad_part = term if grad_part is None else grad_part + term

    grad_core_w = lax.dot_general(
        cores, error, (((0,), (0,)), ((), ())), preferred_element_type=F32
    )
    column = jnp.sum(error.astype(F32), axis=0)
    gain_part = jnp.sum(head_weight.astype(F32) * grad_core_w, axis=1)
    bias_part = jnp.sum(head_weight.astype(F32) * column, axis=1)
    grad_w = grad_core_w * norm_gain[:, None] + norm_bias[:, None] * column
    vector = jnp.concatenate([column, gain_part, bias_part])
    size = vector.shape[0]
    high = vector.astype(BF16)
    low = (vector - high.astype(F32)).astype(BF16)
    extra = -(-2 * size // (width * 16)) * 16
    packed = jnp.concatenate([high, low, jnp.zeros((extra * width - 2 * size,), BF16)])
    packed = packed.reshape(extra, width)
    part = d_s // 8
    grad_w16 = grad_w.astype(BF16)
    dp_at = zh * 4 + y
    own_w = lax.dynamic_slice_in_dim(grad_w, dp_at * part, part, axis=0)
    own_v = [high.astype(F32) + low.astype(F32)]
    for k in range(1, 8):
        block = lax.dynamic_slice_in_dim(grad_w16, (dp_at ^ k) * part, part, axis=0)
        block = jnp.concatenate([block, packed])
        block = lax.ppermute(block, ("zh", "y"), [(i, i ^ k) for i in range(8)]).astype(F32)
        own_w = own_w + block[:part]
        flat = block[part:].reshape(-1)
        own_v.append(flat[:size] + flat[size : 2 * size])
    while len(own_v) > 1:
        own_v = [a + b for a, b in zip(own_v[::2], own_v[1::2])]
    own_v = own_v[0]
    grad_head_w = own_w
    grad_head_b = own_v[:width]
    sums = own_v[width:]

    grad_part = grad_part.reshape(2, rows, d_s)
    keep = lax.dynamic_slice_in_dim(grad_part, zl, 1, axis=0)[0]
    send = lax.dynamic_slice_in_dim(grad_part, 1 - zl, 1, axis=0)[0].astype(BF16)
    grad_normed = keep + moved(send, "zl", 1).astype(F32)
    sums = sums + moved(sums, "zl", 1)
    sums = sums + moved(sums, "c", 1)
    near, over, cross = (
        lax.ppermute(sums, "x", [(i, i ^ k) for i in range(4)]) for k in (1, 2, 3)
    )
    sums = (sums + near) + (over + cross)
    grad_gain, grad_bias = sums[:d_s], sums[d_s:]

    grad_core = grad_normed * norm_gain
    grad_in = inverse * (
        grad_core
        - jnp.mean(grad_core, axis=-1, keepdims=True)
        - core * jnp.mean(grad_core * core, axis=-1, keepdims=True)
    )
    return (grad_head_w, grad_head_b, grad_gain, grad_bias, grad_in)


def solution(mesh):
    split = Mesh(mesh.devices.reshape(2, 4, 4, 2, 2), ("zh", "y", "x", "zl", "c"))
    dp, mp = ("zh", "y"), ("x", "zl", "c")
    placed = (
        P(dp, None),
        P(dp, mp),
        P(dp, mp),
        P(dp, mp),
        P(dp + mp, None),
        P(),
        P(),
        P(None, mp),
        P(mp),
    )
    return jax.shard_map(
        on_device,
        mesh=split,
        in_specs=placed,
        out_specs=(P(dp, mp), P(mp), P(), P(), P(dp + mp, None)),
        check_vma=False,
    )
```
